32 devices in a mesh: section: 4 (over y, core), rep: 2 (over x), tp: 4 (over z).
Axes of the slice: x: 2, y: 2, z: 4, core: 2. Of those that a mesh axis runs over, the one named last changes fastest.
Arguments:
- token_ids: int32 [2, 8, 128], P('rep', None, 'tp'), may hold values from 0 to 16383
- embed: bfloat16 [16384, 1024], P('section'), may hold values from -6 to 6
- w_in: bfloat16 [2, 4, 2, 1024, 2816], P('rep', 'section', None, None, 'tp'), may hold values from -0.1875 to 0.1875
- w_down: bfloat16 [2, 4, 2816, 1024], P('rep', 'section', 'tp'), may hold values from -0.109375 to 0.109375
- outer_in: float32 [4, 2, 1024, 2816], P('section', None, None, 'tp'), may hold values from -0.1875 to 0.1875
- outer_down: float32 [4, 2816, 1024], P('section', 'tp'), may hold values from -0.109375 to 0.109375
- moment_in: float32 [4, 2, 1024, 2816], P('section', None, None, 'tp'), may hold values from -0.12 to 0.12
- moment_down: float32 [4, 2816, 1024], P('section', 'tp'), may hold values from -0.12 to 0.12
- cotangent: bfloat16 [2, 8, 128, 1024], P('rep', None, 'tp'), may hold values from -6 to 6
- fragment: int32 [4], replicated, may hold values 0 or 1
Outputs:
- new_in: bfloat16 [2, 4, 2, 1024, 2816], P('rep', 'section', None, None, 'tp')
- new_down: bfloat16 [2, 4, 2816, 1024], P('rep', 'section', 'tp')
- next_outer_in: float32 [4, 2, 1024, 2816], P('section', None, None, 'tp')
- next_outer_down: float32 [4, 2816, 1024], P('section', 'tp')
- next_moment_in: float32 [4, 2, 1024, 2816], P('section', None, None, 'tp')
- next_moment_down: float32 [4, 2816, 1024], P('section', 'tp')
The draws below stay inside these ranges and needn't reach their ends.
All inputs are finite; a program needn't handle non-finite values.
Results may differ from the reference program's by a relative error of at most 0.03.
Values may be sent and summed in bfloat16 or wider, within the bound.
No kernel may reach another device: no remote copies, remote signals or barrier semaphores. Data moves between devices by JAX's collectives and lax.ppermute only.
A program may use at most 128 MiB of HBM per device.

```python
import math
import jax
import jax.numpy as jnp
import numpy as np
from jax import lax

D = 1024
FF = 2816
VOCAB = 16384
MB = 8
MTOK = 128
LAYERS_SECTION = 1
LAYERS = 4
REPS = 2
N_SECTION = 4


def place_ends(drawn, own_key, low, high):
    dims = drawn.shape
    index_at = [jax.random.randint(jax.random.fold_in(own_key, axis), (), 0, dims[axis]) for axis in range(len(dims))]
    drawn = drawn.at[tuple(index_at)].set(low)
    longest = dims.index(max(dims))
    index_at[longest] = (index_at[longest] + 1) % dims[longest]
    return drawn.at[tuple(index_at)].set(high)


def steps_of(key, shape, shards, smallest, top_value):
    def one(dim, shards_of):
        draws = jax.random.uniform(jax.random.fold_in(jax.random.fold_in(key, 6), dim), (shards_of,), jnp.float32, smallest / len(shards), top_value / len(shards))
        return jnp.repeat(jnp.exp(draws), shape[dim] // shards_of).reshape((-1,) + (1,) * (len(shape) - dim - 1))

    loudness = one(*shards[0])
    for cut in shards[1:]:
        loudness = loudness * one(*cut)
    return loudness


def rank_bounds(number_of, slope):
    loads = [(1 << 20) // math.isqrt(rank ** slope) + 1 for rank in range(1, number_of + 1)]
    scale = 1 + sum(loads) // (1 << 30)
    return np.cumsum(np.array([max(1, weight // scale) for weight in loads]))


def ranked(rng, extent, count, slope):
    listing = rank_bounds(count, slope)
    ticket = jax.random.randint(jax.random.fold_in(rng, 1), extent, 0, int(listing[count - 1]))
    grade = jnp.searchsorted(jnp.asarray(listing, jnp.int32), ticket, side="right")
    return jax.random.permutation(jax.random.fold_in(rng, 2), count)[grade].astype(jnp.int32)


def noise(key, dims, scale, most, shards=(), kind=jnp.bfloat16):
    values = scale * jax.random.normal(key, dims, jnp.float32)
    if shards:
        values = values * steps_of(key, dims, shards, -0.22, 0.18)
    return jnp.clip(values, -most, most).astype(kind)


def setup_inputs(seed: int = 0) -> dict:
    arg_keys = jax.random.split(jax.random.key(seed), 11)
    return {
        "token_ids": place_ends(ranked(arg_keys[0], (REPS, MB, MTOK), VOCAB, 2), jax.random.fold_in(arg_keys[0], 3), 0, VOCAB - 1).astype(jnp.int32),
        "embed": noise(arg_keys[1], (VOCAB, D), 1.0, 6.0, ((0, 4),)),
        "w_in": noise(arg_keys[2], (REPS, LAYERS, 2, D, FF), D ** -0.5, 0.1875, ((0, 2), (1, 4), (4, 4))),
        "w_down": noise(arg_keys[3], (REPS, LAYERS, FF, D), FF ** -0.5, 0.109375, ((0, 2), (1, 4), (2, 4))),
        "outer_in": noise(arg_keys[4], (LAYERS, 2, D, FF), D ** -0.5, 0.1875, ((0, 4), (3, 4)), jnp.float32),
        "outer_down": noise(arg_keys[5], (LAYERS, FF, D), FF ** -0.5, 0.109375, ((0, 4), (1, 4)), jnp.float32),
        "moment_in": noise(arg_keys[6], (LAYERS, 2, D, FF), 0.02, 0.12, ((0, 4), (3, 4)), jnp.float32),
        "moment_down": noise(arg_keys[7], (LAYERS, FF, D), 0.02, 0.12, ((0, 4), (1, 4)), jnp.float32),
        "cotangent": noise(arg_keys[8], (REPS, MB, MTOK, D), 1.0, 6.0, ((0, 2), (2, 4))),
        "fragment": place_ends((jax.random.randint(arg_keys[9], (N_SECTION,), 0, 2) < 1).astype(jnp.int32), jax.random.fold_in(arg_keys[9], 1), 0, 1),
    }


EPS = 1e-05
INNER_LR = 0.001
OUTER_LR = 0.7
MOMENTUM = 0.9

def scale_rows(values):
    return lax.rsqrt(lax.optimization_barrier(jnp.mean(values * values, axis=-1, keepdims=True)) + EPS)

def layer_forward(x, pair, down):
    xf = x.astype(jnp.float32)
    rinv = scale_rows(xf)
    normed = (xf * rinv).astype(jnp.bfloat16)
    gate = jnp.dot(normed, pair[0], preferred_element_type=jnp.float32)
    upper = jnp.dot(normed, pair[1], preferred_element_type=jnp.float32)
    hidden = (jax.nn.silu(gate) * upper).astype(jnp.bfloat16)
    out = jnp.dot(hidden, down, preferred_element_type=jnp.float32)
    return ((xf + out).astype(jnp.bfloat16), (normed, gate, upper, hidden))

def layer_backward(grad, x, pair, down, saved):
    normed, gate, upper, hidden = saved
    d_hidden = jnp.dot(grad, down.T, preferred_element_type=jnp.float32)
    sig = jax.nn.sigmoid(gate)
    d_gate = (d_hidden * upper * sig * (1.0 + gate * (1.0 - sig))).astype(jnp.bfloat16)
    d_upper = (d_hidden * jax.nn.silu(gate)).astype(jnp.bfloat16)
    g_down = jnp.dot(hidden.T, grad, preferred_element_type=jnp.float32)
    g_pair = jnp.stack([jnp.dot(normed.T, d_gate, preferred_element_type=jnp.float32), jnp.dot(normed.T, d_upper, preferred_element_type=jnp.float32)])
    d_norm = jnp.dot(d_gate, pair[0].T, preferred_element_type=jnp.float32) + jnp.dot(d_upper, pair[1].T, preferred_element_type=jnp.float32)
    xf = x.astype(jnp.float32)
    rinv = scale_rows(xf)
    d_x = grad.astype(jnp.float32) + rinv * d_norm - xf * (rinv * rinv * rinv) * lax.optimization_barrier(jnp.mean(d_norm * xf, axis=-1, keepdims=True))
    return (d_x.astype(jnp.bfloat16), g_pair, g_down)

def reference(token_ids, embed, w_in, w_down, outer_in, outer_down, moment_in, moment_down, cotangent, fragment):
    chosen = fragment[jnp.arange(LAYERS) // LAYERS_SECTION] == 1
    inner_in = []
    inner_down = []
    for replica in range(REPS):
        x = jnp.take(embed, token_ids[replica].reshape(-1), axis=0)
        inputs = []
        saves = []
        for layer in range(LAYERS):
            inputs.append(x)
            x, saved = layer_forward(x, w_in[replica, layer], w_down[replica, layer])
            saves.append(saved)
        grad = cotangent[replica].reshape(-1, D)
        pair_list = [None] * LAYERS
        down_list = [None] * LAYERS
        for layer in reversed(range(LAYERS)):
            grad, g_pair, g_down = layer_backward(grad, inputs[layer], w_in[replica, layer], w_down[replica, layer], saves[layer])
            pair_list[layer] = (w_in[replica, layer].astype(jnp.float32) - INNER_LR * g_pair).astype(jnp.bfloat16)
            down_list[layer] = (w_down[replica, layer].astype(jnp.float32) - INNER_LR * g_down).astype(jnp.bfloat16)
        inner_in.append(jnp.stack(pair_list))
        inner_down.append(jnp.stack(down_list))
    inner_in = jnp.stack(inner_in)
    inner_down = jnp.stack(inner_down)
    mean_in = lax.optimization_barrier(jnp.mean(outer_in[None] - inner_in.astype(jnp.float32), axis=0))
    mean_down = lax.optimization_barrier(jnp.mean(outer_down[None] - inner_down.astype(jnp.float32), axis=0))
    moment_next_in = MOMENTUM * moment_in + mean_in
    moment_next_down = MOMENTUM * moment_down + mean_down
    outer_next_in = outer_in - OUTER_LR * (mean_in + MOMENTUM * moment_next_in)
    outer_next_down = outer_down - OUTER_LR * (mean_down + MOMENTUM * moment_next_down)
    pick_in = chosen[:, None, None, None]
    pick_down = chosen[:, None, None]
    new_in = jnp.where(pick_in[None], outer_next_in.astype(jnp.bfloat16)[None], inner_in)
    new_down = jnp.where(pick_down[None], outer_next_down.astype(jnp.bfloat16)[None], inner_down)
    return (new_in, new_down, jnp.where(pick_in, outer_next_in, outer_in), jnp.where(pick_down, outer_next_down, outer_down), jnp.where(pick_in, moment_next_in, moment_in), jnp.where(pick_down, moment_next_down, moment_down))
```

```python
import functools

import jax
import jax.numpy as jnp
from jax import lax
from jax.experimental import pallas as pl
from jax.experimental.pallas import tpu as pltpu
from jax.sharding import PartitionSpec as P


EPS = 1e-05
INNER_LR = 0.001
OUTER_LR = 0.7
MOMENTUM = 0.9
F32 = jnp.float32
BF16 = jnp.bfloat16
VMEM = pl.BlockSpec(memory_space=pltpu.VMEM)
NN = ((1,), (0,))
NT = ((1,), (1,))
TN = ((0,), (0,))


def call(body, outs, args, flops, vmem=20 << 20):
    moved = sum(a.size * a.dtype.itemsize for a in args)
    return pl.pallas_call(
        body,
        out_shape=outs,
        in_specs=[VMEM] * len(args),
        out_specs=[VMEM] * len(outs),
        compiler_params=pltpu.CompilerParams(vmem_limit_bytes=vmem),
        cost_estimate=pl.CostEstimate(flops=flops, bytes_accessed=moved, transcendentals=0),
    )(*args)


def sds(shape, dtype=BF16):
    return jax.ShapeDtypeStruct(shape, dtype)


def dot(a, b, dims):
    return lax.dot_general(a, b, (dims, ((), ())), preferred_element_type=F32)


def rows_scale(x):
    return lax.rsqrt(jnp.mean(x * x, axis=-1, keepdims=True) + EPS)


def lanes(size):
    return -(-size // 128) * 128


def span(width, ff, b):
    at = width + b * lanes(ff)
    return slice(at, at + ff)


def put_parts(outs, value, rows):
    outs[0][...] = value[:rows]
    for k in range(1, len(outs)):
        outs[k][...] = value[k * rows : (k + 1) * rows].astype(BF16)


def part_shapes(tp, rows, width):
    return [sds((rows, width), F32)] + [sds((rows, width))] * (tp - 1)


def norm_body(*refs):
    parts, (x_out, n_out) = refs[:-2], refs[-2:]
    total = parts[0][...]
    for part in parts[1:]:
        total = total + part[...]
    x_out[...] = total
    x = total.astype(F32)
    n_out[...] = (x * rows_scale(x)).astype(BF16)


def norm(parts):
    x = parts[0]
    return call(norm_body, [sds(x.shape), sds(x.shape)], parts, 8 * x.size)


def fwd_body(tp, blocks, down, *refs):
    chunks, refs = refs[:tp], refs[tp:]
    pairs, refs = refs[:blocks], refs[blocks:]
    downs, outs = (refs[:blocks], refs[blocks:]) if down else ((), refs)
    rows = chunks[0].shape[0]
    full = jnp.concatenate([c[...] for c in chunks], axis=0)
    acts_out, gates_out = outs[:2]
    width, ff = full.shape[1], pairs[0].shape[1]
    acts_out[:, :width] = full
    out = None
    for b, pair in enumerate(pairs):
        gate = dot(full, pair[0], NT)
        up = dot(full, pair[1], NT)
        gates_out[2 * b] = gate
        gates_out[2 * b + 1] = up
        hidden = (gate * jax.nn.sigmoid(gate) * up).astype(BF16)
        acts_out[:, span(width, ff, b)] = hidden
        if down:
            term = dot(hidden, downs[b][...], NN)
            out = term if out is None else out + term
    if down:
        put_parts(outs[2:], out, rows)


def fwd_layer(chunks, pairs, downs):
    tp, blocks = len(chunks), len(pairs)
    rows, width = chunks[0].shape
    ff = pairs[0].shape[1]
    outs = [sds((tp * rows, width + blocks * lanes(ff)))]
    outs += [sds((2 * blocks, tp * rows, ff), F32)]
    outs += part_shapes(tp, rows, width) if downs else []
    weights = [*pairs, *downs]
    flops = 2 * tp * rows * sum(w.size for w in weights)
    body = functools.partial(fwd_body, tp, blocks, bool(downs))
    res = call(body, outs, [*chunks, *weights], flops)
    return res[:2], res[2:]


def down_body(blocks, acts, *refs):
    downs, outs = refs[:blocks], refs[blocks:]
    ff, width = downs[0].shape
    out = None
    for b in range(blocks):
        term = dot(acts[:, span(width, ff, b)], downs[b][...], NN)
        out = term if out is None else out + term
    put_parts(outs, out, outs[0].shape[0])


def down_layer(acts, downs, tp):
    tokens, width = acts.shape[0], downs[0].shape[1]
    flops = 2 * tokens * sum(w.size for w in downs)
    body = functools.partial(down_body, len(downs))
    return call(body, part_shapes(tp, tokens // tp, width), [acts, *downs], flops)


def join_body(*refs):
    x_ref, own = refs[:2]
    parts, (x_out, n_out) = refs[2:-2], refs[-2:]
    total = own[...]
    for part in parts:
        total = total + part[...].astype(F32)
    x = (x_ref[...].astype(F32) + total).astype(BF16)
    x_out[...] = x
    xf = x.astype(F32)
    n_out[...] = (xf * rows_scale(xf)).astype(BF16)


def join(x, own, parts):
    return call(join_body, [sds(x.shape), sds(x.shape)], [x, own, *parts], 20 * x.size)


def bwd_body(tp, blocks, last, *refs):
    chunks, gates, refs = refs[:tp], refs[tp], refs[tp + 1 :]
    downs, refs = refs[:blocks], refs[blocks:]
    pairs, outs = ((), refs) if last else (refs[:blocks], refs[blocks:])
    rows = chunks[0].shape[0]
    grad = jnp.concatenate([c[...] for c in chunks], axis=0)
    acts_out = outs[0]
    ff, width = downs[0].shape
    acts_out[:, :width] = grad
    d_norm = None
    for b, down in enumerate(downs):
        d_hidden = dot(grad, down[...], NT)
        gate, up = gates[2 * b], gates[2 * b + 1]
        sig = jax.nn.sigmoid(gate)
        d_gate = (d_hidden * up * sig * (1.0 + gate * (1.0 - sig))).astype(BF16)
        d_up = (d_hidden * (gate * sig)).astype(BF16)
        acts_out[:, span(width, ff, 2 * b)] = d_gate
        acts_out[:, span(width, ff, 2 * b + 1)] = d_up
        if not last:
            term = dot(d_gate, pairs[b][0], NN) + dot(d_up, pairs[b][1], NN)
            d_norm = term if d_norm is None else d_norm + term
    if not last:
        put_parts(outs[1:], d_norm, rows)


def bwd_layer(chunks, gates, pairs, downs, last):
    tp, blocks = len(chunks), len(downs)
    rows, width = chunks[0].shape
    outs = [sds((tp * rows, width + 2 * blocks * lanes(gates.shape[-1])))]
    outs += [] if last else part_shapes(tp, rows, width)
    weights = [*downs] if last else [*downs, *pairs]
    flops = 2 * tp * rows * sum(w.size for w in weights)
    res = call(functools.partial(bwd_body, tp, blocks, last), outs, [*chunks, gates, *weights], flops)
    return res[0], res[1:]


def back_body(*refs):
    g_ref, x_ref, own = refs[:3]
    parts, out = refs[3:-1], refs[-1]
    d_norm = own[...]
    for part in parts:
        d_norm = d_norm + part[...].astype(F32)
    xf = x_ref[...].astype(F32)
    rinv = rows_scale(xf)
    mean = jnp.mean(d_norm * xf, axis=-1, keepdims=True)
    d_x = g_ref[...].astype(F32) + rinv * d_norm - xf * (rinv * rinv * rinv) * mean
    out[...] = d_x.astype(BF16)


def back(grad, x, own, parts):
    return call(back_body, [sds(x.shape)], [grad, x, own, *parts], 20 * x.size)[0]


def wgrad_body(sources, stages, stage_ref, *refs):
    pair_out, down_out = refs[-2:]
    blocks, ff, width = down_out.shape
    stage = stage_ref[0]

    def value(late, source, at):
        out = None
        for s in range(stages):
            one = refs[(late * sources + source) * stages + s][:, at]
            out = one if out is None else jnp.where(stage == s, one, out)
        return out

    def over(late, b, right):
        total = None
        for source in range(sources):
            term = dot(value(late, source, span(width, ff, b)), rights[right][source], TN)
            total = term if total is None else total + term
        return total.astype(BF16)

    top = slice(0, width)
    rights = [[value(late, source, top) for source in range(sources)] for late in range(2)]
    for b in range(blocks):
        pair_out[b, 0] = over(1, 2 * b, 0)
        pair_out[b, 1] = over(1, 2 * b + 1, 0)
        down_out[b] = over(0, b, 1)


def wgrad(stage, blocks, ff, width, acts):
    sources, stages = len(acts[0]), len(acts[0][0])
    outs = [sds((blocks, 2, ff, width)), sds((blocks, ff, width))]
    args = [v for kind in acts for source in kind for v in source]
    flops = 2 * sources * args[0].shape[0] * 3 * blocks * ff * width
    return pl.pallas_call(
        functools.partial(wgrad_body, sources, stages),
        out_shape=outs,
        in_specs=[pl.BlockSpec(memory_space=pltpu.SMEM)] + [VMEM] * len(args),
        out_specs=[VMEM] * 2,
        compiler_params=pltpu.CompilerParams(vmem_limit_bytes=40 << 20),
        cost_estimate=pl.CostEstimate(flops=flops, bytes_accessed=flops // 512, transcendentals=0),
    )(stage.astype(jnp.int32).reshape(1), *args)


def settle_body(flip, w_ref, own, *refs):
    other, out = refs if len(refs) == 2 else (None, refs[0])
    blocks = own.shape[0]
    size = own.shape[-2]
    for b in range(blocks):
        g = own[b].astype(F32)
        if other is not None:
            g = g + other[blocks - 1 - b].astype(F32)
        h = blocks - 1 - b if flip else b
        at = (Ellipsis, slice(h * size, (h + 1) * size), slice(None))
        out[at] = (w_ref[at].astype(F32) - INNER_LR * g).astype(BF16)


def settle(w, own, others, flip):
    body = functools.partial(settle_body, flip)
    return call(body, [sds(w.shape)], [w, own, *others], 4 * w.size, 40 << 20)[0]


def after(value, *others):
    return lax.optimization_barrier((value, others))[0]


def spread(value):
    tp = lax.axis_size("tp")
    return [value] + [
        lax.ppermute(value, "tp", [(i, (i + k) % tp) for i in range(tp)]) for k in range(1, tp)
    ]


def collect(parts):
    tp = lax.axis_size("tp")
    return [
        lax.ppermute(parts[k], "tp", [(i, (i - k) % tp) for i in range(tp)]) for k in range(1, tp)
    ]


def choose(index, values):
    out = values[0]
    for i, value in enumerate(values[1:], 1):
        out = jnp.where(index == i, value, out)
    return out


def shards(
    token_ids,
    embed,
    w_in,
    w_down,
    outer_in,
    outer_down,
    moment_in,
    moment_down,
    cotangent,
    fragment,
):
    sections = lax.axis_size("section")
    section = lax.axis_index("section")
    replicas = lax.axis_size("rep")
    group = 2 if sections % 2 == 0 else 1
    stages = sections // group
    stage, core = section // group, section % group
    shifts = range(1, stages)
    width = embed.shape[1]
    even = core == 0

    def swap(value):
        return lax.ppermute(value, "section", [(s, s ^ 1) for s in range(sections)])

    def shift(value, j):
        pairs = [(s, (s + j * group) % sections) for s in range(sections)]
        return lax.ppermute(value, "section", pairs)

    def to_member(value, member):
        pairs = [(s * group + 1 - member, s * group + member) for s in range(stages)]
        return lax.ppermute(value, "section", pairs)

    pairs = jnp.swapaxes(w_in[0], -1, -2)
    downs = w_down[0]
    depth = pairs.shape[0]
    ff = downs.shape[1]
    block = ff // group

    def cut(value, index):
        return lax.dynamic_slice_in_dim(value, index * block, block, value.ndim - 2)

    own = [pairs, downs]
    if group == 2:
        mine = [cut(w, core) for w in own]
        theirs = [cut(w, 1 - core) for w in own]
        away = [swap(w) for w in theirs]
        homes = [
            [jnp.where(even, m, a) for m, a in zip(mine, away)],
            [jnp.where(even, a, m) for m, a in zip(mine, away)],
        ]
    else:
        theirs, homes = own, [own]
    gathered = [[None, None] for _ in homes]

    def gather_weights(g, kind, ready):
        w = after(homes[g][kind], ready)
        gathered[g][kind] = [w] + [shift(w, j) for j in shifts]

    gather_weights(0, 0, theirs)

    def layer_weights(s, g, kind, ready):
        parts = gathered[g][kind]
        parts = [parts[0]] + [after(w, ready) for w in parts[1:]]
        ordered = choose((stage - s) % stages, parts)
        both = [ordered] + ([swap(ordered)] if group == 2 else [])
        return [[w[d] for w in both] for d in range(depth)]

    ids = token_ids[0].reshape(stages, group, -1)
    rows = ids.shape[-1]
    ids = lax.dynamic_slice_in_dim(jnp.concatenate([ids, ids], axis=0), stage, stages, 0)
    ids = lax.dynamic_slice_in_dim(jnp.concatenate([ids, ids], axis=1), core, group, 1)
    ids = jnp.swapaxes(ids, 0, 1).reshape(-1)
    vocab_part = embed.shape[0]
    local_ids = after(ids, *theirs) - section * vocab_part
    inside = (local_ids >= 0) & (local_ids < vocab_part)
    looked = jnp.take(embed, jnp.clip(local_ids, 0, vocab_part - 1), axis=0)
    looked = jnp.where(inside[:, None], looked, jnp.zeros((), BF16))
    if group == 2:
        split = stages * rows
        looked = looked[:split] + swap(looked[split:])
    gather_weights(0, 1, looked)
    seeds = cotangent[0].reshape(-1, width)
    grad = lax.dynamic_slice_in_dim(seeds, section * rows, rows, 0)
    seed_chunks = spread(grad)
    looks = [shift(looked[j * rows : (j + 1) * rows], j) for j in shifts]
    for g in range(1, group):
        gather_weights(g, 0, looked)
        gather_weights(g, 1, looked)
    x, normed = norm([looked[:rows]] + looks)

    count = stages * group * depth
    saved, xs, layers = [], [], []
    for l in range(count):
        s, g, d = l // (group * depth), l // depth % group, l % depth
        xs.append(x)
        chunks = spread(normed)
        if d == 0:
            ready = normed if l == 0 else chunks if l < group * depth else before
            by_kind = [layer_weights(s, g, 0, ready), layer_weights(s, g, 1, chunks)]
        before = chunks
        if l == 0:
            kept, _ = fwd_layer(chunks, by_kind[0][d], [])
            parts = down_layer(kept[0], by_kind[1][d], len(chunks))
        else:
            downs_used = by_kind[1][d] if l < count - 1 else []
            kept, parts = fwd_layer(chunks, by_kind[0][d], downs_used)
        layers.append((by_kind[0][d], by_kind[1][d]))
        saved.append(kept)
        if l < count - 1:
            x, normed = join(x, parts[0], collect(parts))

    def to_home(value, s):
        out = [value]
        for j in shifts:
            t = (s + j) % stages
            pairs = [(t * group + g, s * group + g) for g in range(group)]
            out.append(lax.ppermute(value, "section", pairs))
        return out

    acts = []
    for l in range(count):
        acts.append([to_home(saved[l][0], l // (group * depth))])

    def grads_of(g):
        sets = []
        for d in range(depth):
            of = [acts[(s * group + g) * depth + d] for s in range(stages)]
            kinds = [[[a[kind][j] for a in of] for j in range(stages)] for kind in range(2)]
            sets.append(wgrad(stage, group, block, width, kinds))
        out = []
        for i in range(2):
            own = jnp.stack([one[i] for one in sets], axis=1)
            out.append((own, [to_member(own, g)] if group == 2 else []))
        return out

    sums = [None] * group
    for l in reversed(range(count)):
        gates = saved[l][1]
        chunks = seed_chunks if l == count - 1 else spread(grad)
        if l == group * depth - 1:
            gates = after(gates, *[v for a in acts for kind in a[:1] for v in kind[1:]])
        if (l + 1) % depth == 0 and 0 < (l + 1) // depth < group:
            for a in acts[l + 1 :]:
                a[1][1:] = [after(v, grad) for v in a[1][1:]]
            sums[(l + 1) // depth] = grads_of((l + 1) // depth)
            gates = after(gates, *[own for own, _ in sums[(l + 1) // depth]])
        late, parts = bwd_layer(chunks, gates, *layers[l], l == 0)
        acts[l].append(to_home(late, l // (group * depth)))
        if l > 0:
            grad = back(grad, xs[l], parts[0], collect(parts))

    starts = [pairs, downs]

    def exchange(inner, member):
        if replicas != 2:
            every = lax.all_gather(inner, "rep", axis=0).astype(F32)
            return jnp.sum(every, axis=0) - inner.astype(F32)
        ring = [
            ((s * group + member) * 2 + r, (s * group + member) * 2 + 1 - r)
            for s in range(stages)
            for r in range(2)
        ]
        return lax.ppermute(inner, ("section", "rep"), ring)

    inners, others = [[], []], [[], []]
    ready = acts[0][1][0]
    for g in reversed(range(group)):
        if sums[g] is None:
            for a in acts:
                a[1][1:] = [after(v, ready) for v in a[1][1:]]
            sums[g] = grads_of(g)
        for i, (own, away) in enumerate(sums[g]):
            away = [after(v, ready) for v in away]
            inner = settle(starts[i], own, away, g > 0)
            inners[i].insert(0, inner)
            others[i].insert(0, exchange(inner, g))
            ready = inner

    flag = lax.dynamic_index_in_dim(fragment, section, 0, keepdims=False)
    chosen = flag == 1

    def finish(i, outer, moment):
        inner = choose(core, inners[i])
        total = inner.astype(F32) + choose(core, others[i]).astype(F32)
        mean = outer - total / replicas
        next_moment = MOMENTUM * moment + mean
        next_outer = outer - OUTER_LR * (mean + MOMENTUM * next_moment)
        return (
            jnp.where(chosen, next_outer.astype(BF16), inner),
            jnp.where(chosen, next_outer, outer),
            jnp.where(chosen, next_moment, moment),
        )

    flip = lambda v: jnp.swapaxes(v, -1, -2)
    new_in, next_in, next_m_in = finish(0, flip(outer_in), flip(moment_in))
    outer_down, moment_down = after((outer_down, moment_down), next_in)
    new_down, next_down, next_m_down = finish(1, outer_down, moment_down)
    return (
        flip(new_in)[None],
        new_down[None],
        flip(next_in),
        next_down,
        flip(next_m_in),
        next_m_down,
    )


def solution(mesh):
    return jax.shard_map(
        shards,
        mesh=mesh,
        in_specs=(
            P("rep", None, "tp"),
            P("section", None),
            P("rep", "section", None, None, "tp"),
            P("rep", "section", "tp", None),
            P("section", None, None, "tp"),
            P("section", "tp", None),
            P("section", None, None, "tp"),
            P("section", "tp", None),
            P("rep", None, "tp", None),
            P(),
        ),
        out_specs=(
            P("rep", "section", None, None, "tp"),
            P("rep", "section", "tp", None),
            P("section", None, None, "tp"),
            P("section", "tp", None),
            P("section", None, None, "tp"),
            P("section", "tp", None),
        ),
        check_vma=False,
    )
```

```python
import functools
import math

import jax
import jax.numpy as jnp
from jax import lax
from jax.experimental import pallas as pl
from jax.experimental.pallas import tpu as pltpu
from jax.sharding import PartitionSpec as P


EPS = 1e-05
INNER_LR = 0.001
OUTER_LR = 0.7
MOMENTUM = 0.9
F32 = jnp.float32
BF16 = jnp.bfloat16
VMEM = pl.BlockSpec(memory_space=pltpu.VMEM)
NN = ((1,), (0,))
NT = ((1,), (1,))
TN = ((0,), (0,))


def call(body, outs, args, flops, vmem=12 << 20):
    moved = sum(a.size * a.dtype.itemsize for a in args)
    return pl.pallas_call(
        body,
        out_shape=outs,
        in_specs=[VMEM] * len(args),
        out_specs=[VMEM] * len(outs),
        compiler_params=pltpu.CompilerParams(vmem_limit_bytes=vmem),
        cost_estimate=pl.CostEstimate(flops=flops, bytes_accessed=moved, transcendentals=0),
    )(*args)


def sds(shape, dtype=BF16):
    return jax.ShapeDtypeStruct(shape, dtype)


def dot(a, b, dims):
    return lax.dot_general(a, b, (dims, ((), ())), preferred_element_type=F32)


def rows_scale(x):
    return lax.rsqrt(jnp.mean(x * x, axis=-1, keepdims=True) + EPS)


def lanes(size):
    return -(-size // 128) * 128


def span(width, ff, b):
    at = width + b * lanes(ff)
    return slice(at, at + ff)


def put_parts(outs, value, rows):
    outs[0][...] = value[:rows]
    for k in range(1, len(outs)):
        outs[k][...] = value[k * rows : (k + 1) * rows].astype(BF16)


def part_shapes(tp, rows, width):
    return [sds((rows, width), F32)] + [sds((rows, width))] * (tp - 1)


def norm_body(*refs):
    parts, (x_out, n_out) = refs[:-2], refs[-2:]
    total = parts[0][...]
    for part in parts[1:]:
        total = total + part[...]
    x_out[...] = total
    x = total.astype(F32)
    n_out[...] = (x * rows_scale(x)).astype(BF16)


def norm(parts):
    x = parts[0]
    return call(norm_body, [sds(x.shape), sds(x.shape)], parts, 8 * x.size)


def fwd_body(tp, blocks, down, *refs):
    chunks, refs = refs[:tp], refs[tp:]
    pairs, refs = refs[:blocks], refs[blocks:]
    downs, outs = (refs[:blocks], refs[blocks:]) if down else ((), refs)
    rows = chunks[0].shape[0]
    full = jnp.concatenate([c[...] for c in chunks], axis=0)
    acts_out, gates_out = outs[:2]
    width, ff = full.shape[1], pairs[0].shape[1]
    acts_out[:, :width] = full
    out = None
    for b, pair in enumerate(pairs):
        gate = dot(full, pair[0], NT)
        up = dot(full, pair[1], NT)
        gates_out[2 * b] = gate
        gates_out[2 * b + 1] = up
        hidden = (gate * jax.nn.sigmoid(gate) * up).astype(BF16)
        acts_out[:, span(width, ff, b)] = hidden
        if down:
            term = dot(hidden, downs[b][...], NN)
            out = term if out is None else out + term
    if down:
        put_parts(outs[2:], out, rows)


def fwd_layer(chunks, pairs, downs):
    tp, blocks = len(chunks), len(pairs)
    rows, width = chunks[0].shape
    ff = pairs[0].shape[1]
    outs = [sds((tp * rows, width + blocks * lanes(ff)))]
    outs += [sds((2 * blocks, tp * rows, ff), F32)]
    outs += part_shapes(tp, rows, width) if downs else []
    weights = [*pairs, *downs]
    flops = 2 * tp * rows * sum(w.size for w in weights)
    body = functools.partial(fwd_body, tp, blocks, bool(downs))
    res = call(body, outs, [*chunks, *weights], flops)
    return res[:2], res[2:]


def down_body(blocks, acts, *refs):
    downs, outs = refs[:blocks], refs[blocks:]
    ff, width = downs[0].shape
    out = None
    for b in range(blocks):
        term = dot(acts[:, span(width, ff, b)], downs[b][...], NN)
        out = term if out is None else out + term
    put_parts(outs, out, outs[0].shape[0])


def down_layer(acts, downs, tp):
    tokens, width = acts.shape[0], downs[0].shape[1]
    flops = 2 * tokens * sum(w.size for w in downs)
    body = functools.partial(down_body, len(downs))
    return call(body, part_shapes(tp, tokens // tp, width), [acts, *downs], flops)


def join_body(*refs):
    x_ref, own = refs[:2]
    parts, (x_out, n_out) = refs[2:-2], refs[-2:]
    total = own[...]
    for part in parts:
        total = total + part[...].astype(F32)
    x = (x_ref[...].astype(F32) + total).astype(BF16)
    x_out[...] = x
    xf = x.astype(F32)
    n_out[...] = (xf * rows_scale(xf)).astype(BF16)


def join(x, own, parts):
    return call(join_body, [sds(x.shape), sds(x.shape)], [x, own, *parts], 20 * x.size)


def gather_body(*refs):
    refs[-1][...] = jnp.concatenate([c[...] for c in refs[:-1]], axis=0)


def gather(chunks):
    rows, width = chunks[0].shape
    return call(gather_body, [sds((len(chunks) * rows, width))], chunks, 1 << 20)[0]


def bwd_body(tp, blocks, last, grad_ref, gates, *refs):
    downs, refs = refs[:blocks], refs[blocks:]
    pairs, outs = ((), refs) if last else (refs[:blocks], refs[blocks:])
    grad = grad_ref[...]
    rows = grad.shape[0] // tp
    acts_out = outs[0]
    ff = downs[0].shape[0]
    d_norm = None
    for b, down in enumerate(downs):
        d_hidden = dot(grad, down[...], NT)
        gate, up = gates[2 * b], gates[2 * b + 1]
        sig = jax.nn.sigmoid(gate)
        d_gate = (d_hidden * up * sig * (1.0 + gate * (1.0 - sig))).astype(BF16)
        d_up = (d_hidden * (gate * sig)).astype(BF16)
        acts_out[:, span(0, ff, 2 * b)] = d_gate
        acts_out[:, span(0, ff, 2 * b + 1)] = d_up
        if not last:
            term = dot(d_gate, pairs[b][0], NN) + dot(d_up, pairs[b][1], NN)
            d_norm = term if d_norm is None else d_norm + term
    if not last:
        put_parts(outs[1:], d_norm, rows)


def bwd_layer(grad, gates, pairs, downs, tp, last):
    blocks = len(downs)
    rows, width = grad.shape[0] // tp, grad.shape[1]
    outs = [sds((tp * rows, 2 * blocks * lanes(gates.shape[-1])))]
    outs += [] if last else part_shapes(tp, rows, width)
    weights = [*downs] if last else [*downs, *pairs]
    flops = 2 * tp * rows * sum(w.size for w in weights)
    res = call(functools.partial(bwd_body, tp, blocks, last), outs, [grad, gates, *weights], flops)
    return res[0], res[1:]


def back_body(*refs):
    g_ref, x_ref, own = refs[:3]
    parts, out = refs[3:-1], refs[-1]
    d_norm = own[...]
    for part in parts:
        d_norm = d_norm + part[...].astype(F32)
    xf = x_ref[...].astype(F32)
    rinv = rows_scale(xf)
    mean = jnp.mean(d_norm * xf, axis=-1, keepdims=True)
    d_x = g_ref[...].astype(F32) + rinv * d_norm - xf * (rinv * rinv * rinv) * mean
    out[...] = d_x.astype(BF16)


def back(grad, x, own, parts):
    return call(back_body, [sds(x.shape)], [grad, x, own, *parts], 20 * x.size)[0]


def wgrad_body(sources, stages, base, stage_ref, *refs):
    out = refs[-1]
    blocks, kinds, ff, width = out.shape
    stage = stage_ref[0]

    def value(side, source, at):
        picked = None
        for s in range(stages):
            one = refs[(side * sources + source) * stages + s][:, at]
            picked = one if picked is None else jnp.where(stage == s, one, picked)
        return picked

    rights = [value(1, source, slice(0, width)) for source in range(sources)]
    for b in range(blocks):
        for kind in range(kinds):
            total = None
            for source in range(sources):
                left = value(0, source, span(base, ff, kinds * b + kind))
                term = dot(left, rights[source], TN)
                total = term if total is None else total + term
            out[b, kind] = total.astype(BF16)


def wgrad(stage, shape, base, lefts, rights):
    sources, stages = len(lefts), len(lefts[0])
    args = [v for side in (lefts, rights) for source in side for v in source]
    flops = 2 * sources * args[0].shape[0] * math.prod(shape)
    return pl.pallas_call(
        functools.partial(wgrad_body, sources, stages, base),
        out_shape=sds(shape),
        in_specs=[pl.BlockSpec(memory_space=pltpu.SMEM)] + [VMEM] * len(args),
        out_specs=VMEM,
        compiler_params=pltpu.CompilerParams(vmem_limit_bytes=32 << 20),
        cost_estimate=pl.CostEstimate(flops=flops, bytes_accessed=flops // 512, transcendentals=0),
    )(stage.astype(jnp.int32).reshape(1), *args)


def tile_rows(size, most=176):
    return max(r for r in range(16, most + 1, 16) if size % r == 0)


def settle_body(flip, blocks, w_ref, own, *refs):
    other, outs = (refs[0], refs[1:]) if blocks == 2 else (None, refs)
    kinds, depth = len(outs), outs[0].shape[0]
    size = own.shape[-2]
    step = tile_rows(size, 48)
    for d in range(depth):
        for kind in range(kinds):
            for b in range(blocks):
                h = blocks - 1 - b if flip else b

                @pl.loop(0, size // step)
                def _(i):
                    at = pl.ds(pl.multiple_of(i * step, 16), step)
                    to = pl.ds(pl.multiple_of(h * size + i * step, 16), step)
                    g = own[b, d, kind, at, :].astype(F32)
                    if other is not None:
                        g = g + other[blocks - 1 - b, d, kind, at, :].astype(F32)
                    w = w_ref[d, kind, to, :].astype(F32)
                    outs[kind][d, to, :] = (w - INNER_LR * g).astype(BF16)


def settle(w, own, others, flip):
    depth, kinds, size, width = w.shape
    body = functools.partial(settle_body, flip, own.shape[0])
    outs = [sds((depth, size, width))] * kinds
    return call(body, outs, [w, own, *others], 4 * w.size, 40 << 20)


def update_body(replicas, group, info, *refs):
    inners, others = refs[:group], refs[group : 2 * group]
    outer_ref, moment_ref = refs[2 * group : 2 * group + 2]
    new_out, outer_out, moment_out = refs[-3:]
    core, chosen = info[0], info[1] == 1

    @pl.loop(0, outer_ref.shape[2] // 16)
    def _(i):
        at = pl.ds(pl.multiple_of(i * 16, 16), 16)
        inner, other = inners[0][0, at, :], others[0][0, at, :]
        for g in range(1, group):
            inner = jnp.where(core == g, inners[g][0, at, :], inner)
            other = jnp.where(core == g, others[g][0, at, :], other)
        outer, moment = outer_ref[0, 0, at, :], moment_ref[0, 0, at, :]
        mean = outer - (inner.astype(F32) + other.astype(F32)) / replicas
        next_moment = MOMENTUM * moment + mean
        next_outer = outer - OUTER_LR * (mean + MOMENTUM * next_moment)
        new_out[0, 0, at, :] = jnp.where(chosen, next_outer.astype(BF16), inner)
        outer_out[0, 0, at, :] = jnp.where(chosen, next_outer, outer)
        moment_out[0, 0, at, :] = jnp.where(chosen, next_moment, moment)


def update(info, kind, replicas, inners, others, outer, moment, done):
    group = len(inners)
    depth, kinds, size, width = outer.shape
    rows = tile_rows(size)

    def member(g):
        def at(d, i, info):
            mine = info[0] == g
            return (jnp.where(mine, d, 0), jnp.where(mine, i, 0), 0)

        return pl.BlockSpec((1, rows, width), at)

    whole = pl.BlockSpec((1, 1, rows, width), lambda d, i, info: (d, kind, i, 0))
    specs = [member(g) for g in range(group)] * 2 + [whole] * 2
    specs += [pl.BlockSpec(memory_space=pl.ANY)] * len(done)
    first = 1 + 2 * group + 2
    return pl.pallas_call(
        functools.partial(update_body, replicas, group),
        out_shape=[sds(outer.shape), sds(outer.shape, F32), sds(outer.shape, F32)],
        grid_spec=pltpu.PrefetchScalarGridSpec(
            num_scalar_prefetch=1,
            grid=(depth, size // rows),
            in_specs=specs,
            out_specs=[whole] * 3,
        ),
        input_output_aliases={first + i: i for i in range(len(done))},
        compiler_params=pltpu.CompilerParams(vmem_limit_bytes=60 << 20),
        cost_estimate=pl.CostEstimate(
            flops=10 * outer.size // kinds,
            bytes_accessed=22 * outer.size // kinds,
            transcendentals=0,
        ),
    )(info, *inners, *others, outer, moment, *done)


def after(value, *others):
    return lax.optimization_barrier((value, others))[0]


def spread(value):
    tp = lax.axis_size("tp")
    return [value] + [
        lax.ppermute(value, "tp", [(i, (i + k) % tp) for i in range(tp)]) for k in range(1, tp)
    ]


def collect(parts):
    tp = lax.axis_size("tp")
    return [
        lax.ppermute(parts[k], "tp", [(i, (i - k) % tp) for i in range(tp)]) for k in range(1, tp)
    ]


def choose(index, values):
    out = values[0]
    for i, value in enumerate(values[1:], 1):
        out = jnp.where(index == i, value, out)
    return out


def shards(
    token_ids,
    embed,
    w_in,
    w_down,
    outer_in,
    outer_down,
    moment_in,
    moment_down,
    cotangent,
    fragment,
):
    sections = lax.axis_size("section")
    section = lax.axis_index("section")
    replicas = lax.axis_size("rep")
    group = 2 if sections % 2 == 0 else 1
    stages = sections // group
    stage, core = section // group, section % group
    shifts = range(1, stages)
    width = embed.shape[1]
    even = core == 0

    def swap(value):
        return lax.ppermute(value, "section", [(s, s ^ 1) for s in range(sections)])

    def shift(value, j):
        pairs = [(s, (s + j * group) % sections) for s in range(sections)]
        return lax.ppermute(value, "section", pairs)

    def to_member(value, member):
        pairs = [(s * group + 1 - member, s * group + member) for s in range(stages)]
        return lax.ppermute(value, "section", pairs)

    pairs = jnp.swapaxes(w_in[0], -1, -2)
    downs = w_down[0]
    depth = pairs.shape[0]
    ff = downs.shape[1]
    block = ff // group

    def cut(value, index):
        return lax.dynamic_slice_in_dim(value, index * block, block, value.ndim - 2)

    own = [pairs, downs]
    if group == 2:
        mine = [cut(w, core) for w in own]
        theirs = [cut(w, 1 - core) for w in own]
        away = [swap(w) for w in theirs]
        homes = [
            [jnp.where(even, m, a) for m, a in zip(mine, away)],
            [jnp.where(even, a, m) for m, a in zip(mine, away)],
        ]
    else:
        theirs, homes = own, [own]
    gathered = [[None, None] for _ in homes]

    def gather_weights(g, kind, ready):
        w = after(homes[g][kind], ready)
        gathered[g][kind] = [w] + [shift(w, j) for j in shifts]

    gather_weights(0, 0, theirs)

    def layer_weights(s, g, kind, ready):
        parts = gathered[g][kind]
        parts = [parts[0]] + [after(w, ready) for w in parts[1:]]
        ordered = choose((stage - s) % stages, parts)
        both = [ordered] + ([swap(ordered)] if group == 2 else [])
        return [[w[d] for w in both] for d in range(depth)]

    ids = token_ids[0].reshape(stages, group, -1)
    rows = ids.shape[-1]
    ids = lax.dynamic_slice_in_dim(jnp.concatenate([ids, ids], axis=0), stage, stages, 0)
    ids = lax.dynamic_slice_in_dim(jnp.concatenate([ids, ids], axis=1), core, group, 1)
    ids = jnp.swapaxes(ids, 0, 1).reshape(-1)
    vocab_part = embed.shape[0]
    local_ids = after(ids, *theirs) - section * vocab_part
    inside = (local_ids >= 0) & (local_ids < vocab_part)
    looked = jnp.take(embed, jnp.clip(local_ids, 0, vocab_part - 1), axis=0)
    looked = jnp.where(inside[:, None], looked, jnp.zeros((), BF16))
    if group == 2:
        split = stages * rows
        looked = looked[:split] + swap(looked[split:])
    gather_weights(0, 1, looked)
    seeds = cotangent[0].reshape(-1, width)
    grad = lax.dynamic_slice_in_dim(seeds, section * rows, rows, 0)
    seed_chunks = spread(grad)
    looks = [shift(looked[j * rows : (j + 1) * rows], j) for j in shifts]
    for g in range(1, group):
        gather_weights(g, 0, looked)
        gather_weights(g, 1, looked)
    x, normed = norm([looked[:rows]] + looks)

    count = stages * group * depth
    saved, xs, layers = [], [], []
    for l in range(count):
        s, g, d = l // (group * depth), l // depth % group, l % depth
        xs.append(x)
        chunks = spread(normed)
        if d == 0:
            ready = normed if l == 0 else chunks if l < group * depth else before
            by_kind = [layer_weights(s, g, 0, ready), layer_weights(s, g, 1, chunks)]
        before = chunks
        if l == 0:
            kept, _ = fwd_layer(chunks, by_kind[0][d], [])
            parts = down_layer(kept[0], by_kind[1][d], len(chunks))
        else:
            downs_used = by_kind[1][d] if l < count - 1 else []
            kept, parts = fwd_layer(chunks, by_kind[0][d], downs_used)
        layers.append((by_kind[0][d], by_kind[1][d]))
        saved.append(kept)
        if l < count - 1:
            collected = collect(parts)
            x, normed = join(x, parts[0], collected)

    def to_home(value, s):
        out = [value]
        for j in shifts:
            t = (s + j) % stages
            pairs = [(t * group + g, s * group + g) for g in range(group)]
            out.append(lax.ppermute(value, "section", pairs))
        return out

    acts = []
    for l in range(count):
        acts.append([to_home(saved[l][0], l // (group * depth))])

    def grads_of(g, pair, ready):
        sets = []
        for d in range(depth):
            of = [acts[(s * group + g) * depth + d] for s in range(stages)]
            kinds = [[[a[kind][j] for a in of] for j in range(stages)] for kind in range(3 if pair else 2)]
            kinds[-1][1:] = [[after(v, ready) for v in one] for one in kinds[-1][1:]]
            if pair:
                shape = (group, 2, block, width)
                sets.append(wgrad(stage, shape, 0, kinds[2], kinds[0]))
            else:
                shape = (group, 1, block, width)
                sets.append(wgrad(stage, shape, width, kinds[0], kinds[1]))
        own = jnp.stack(sets, axis=1)
        return own, [to_member(own, g)] if group == 2 else []

    sums = {}
    for l in reversed(range(count)):
        s, g = l // (group * depth), (l + 1) // depth
        gates = saved[l][1]
        chunks = seed_chunks if l == count - 1 else spread(grad)
        if l == group * depth - 1:
            gates = after(gates, *[v for a in acts for v in a[0][1:]])
        whole = gather(chunks)
        acts[l].append(to_home(whole, s))
        if (l + 1) % depth == 0 and 0 < g < group:
            sums[g, True] = grads_of(g, True, grad)
            gates = after(gates, sums[g, True][0])
        late, parts = bwd_layer(whole, gates, *layers[l], len(chunks), l == 0)
        acts[l].append(to_home(late, s))
        if l < group * depth and l % depth == 0:
            sums[l // depth, False] = grads_of(l // depth, False, late)
        if l > 0:
            collected = collect(parts)
            grad = back(grad, xs[l], parts[0], collected)

    starts = [pairs, downs[:, None]]

    def exchange(inner, member):
        if replicas != 2:
            every = lax.all_gather(inner, "rep", axis=0).astype(F32)
            return jnp.sum(every, axis=0) - inner.astype(F32)
        ring = [
            ((s * group + member) * 2 + r, (s * group + member) * 2 + 1 - r)
            for s in range(stages)
            for r in range(2)
        ]
        return lax.ppermute(inner, ("section", "rep"), ring)

    inners, others = [[], [], []], [[], [], []]
    sums[0, True] = grads_of(0, True, acts[0][2][0])
    for g in reversed(range(group)):
        for i in (1, 0):
            own, away = sums[g, i == 0]
            settled = settle(starts[i], own, away, g > 0)
            for j, inner in enumerate(settled, 2 * i):
                inners[j].insert(0, inner)
                others[j].insert(0, exchange(inner, g))

    info = jnp.stack([core, lax.dynamic_index_in_dim(fragment, section, 0, keepdims=False)])

    def finish(kind, first, outer, moment, done):
        at = kind - first
        return update(info, at, replicas, inners[kind], others[kind], outer, moment, done)

    flip = lambda v: jnp.swapaxes(v, -1, -2)
    outer_in, moment_in = flip(outer_in), flip(moment_in)
    outer_down, moment_down = outer_down[:, None], moment_down[:, None]
    new_down, next_down, next_m_down = finish(2, 2, outer_down, moment_down, [])
    outer_in, moment_in = after((outer_in, moment_in), next_down)
    done = finish(0, 0, outer_in, moment_in, [])
    new_in, next_in, next_m_in = finish(1, 0, outer_in, moment_in, done)
    return (
        flip(new_in)[None],
        new_down[None, :, 0],
        flip(next_in),
        next_down[:, 0],
        flip(next_m_in),
        next_m_down[:, 0],
    )


def solution(mesh):
    return jax.shard_map(
        shards,
        mesh=mesh,
        in_specs=(
            P("rep", None, "tp"),
            P("section", None),
            P("rep", "section", None, None, "tp"),
            P("rep", "section", "tp", None),
            P("section", None, None, "tp"),
            P("section", "tp", None),
            P("section", None, None, "tp"),
            P("section", "tp", None),
            P("rep", None, "tp", None),
            P(),
        ),
        out_specs=(
            P("rep", "section", None, None, "tp"),
            P("rep", "section", "tp", None),
            P("section", None, None, "tp"),
            P("section", "tp", None),
            P("section", None, None, "tp"),
            P("section", "tp", None),
        ),
        check_vma=False,
    )
```

```python
import functools
import math

import jax
import jax.numpy as jnp
from jax import lax
from jax.experimental import pallas as pl
from jax.experimental.pallas import tpu as pltpu
from jax.sharding import PartitionSpec as P


EPS = 1e-05
INNER_LR = 0.001
OUTER_LR = 0.7
MOMENTUM = 0.9
F32 = jnp.float32
BF16 = jnp.bfloat16
VMEM = pl.BlockSpec(memory_space=pltpu.VMEM)
NN = ((1,), (0,))
NT = ((1,), (1,))
TN = ((0,), (0,))


def call(body, outs, args, flops, vmem=12 << 20):
    moved = sum(a.size * a.dtype.itemsize for a in args)
    return pl.pallas_call(
        body,
        out_shape=outs,
        in_specs=[VMEM] * len(args),
        out_specs=[VMEM] * len(outs),
        compiler_params=pltpu.CompilerParams(vmem_limit_bytes=vmem),
        cost_estimate=pl.CostEstimate(flops=flops, bytes_accessed=moved, transcendentals=0),
    )(*args)


def sds(shape, dtype=BF16):
    return jax.ShapeDtypeStruct(shape, dtype)


def dot(a, b, dims):
    return lax.dot_general(a, b, (dims, ((), ())), preferred_element_type=F32)


def rows_scale(x):
    return lax.rsqrt(jnp.mean(x * x, axis=-1, keepdims=True) + EPS)


def lanes(size):
    return -(-size // 128) * 128


def span(width, ff, b):
    at = width + b * lanes(ff)
    return slice(at, at + ff)


def put_parts(outs, value, rows):
    outs[0][...] = value[:rows]
    for k in range(1, len(outs)):
        outs[k][...] = value[k * rows : (k + 1) * rows].astype(BF16)


def part_shapes(tp, rows, width):
    return [sds((rows, width), F32)] + [sds((rows, width))] * (tp - 1)


def norm_body(*refs):
    parts, (x_out, n_out) = refs[:-2], refs[-2:]
    total = parts[0][...]
    for part in parts[1:]:
        total = total + part[...]
    x_out[...] = total
    x = total.astype(F32)
    n_out[...] = (x * rows_scale(x)).astype(BF16)


def norm(parts):
    x = parts[0]
    return call(norm_body, [sds(x.shape), sds(x.shape)], parts, 8 * x.size)


def fwd_body(tp, blocks, down, *refs):
    chunks, refs = refs[:tp], refs[tp:]
    pairs, refs = refs[:blocks], refs[blocks:]
    downs, outs = (refs[:blocks], refs[blocks:]) if down else ((), refs)
    rows = chunks[0].shape[0]
    full = jnp.concatenate([c[...] for c in chunks], axis=0)
    acts_out, gates_out = outs[:2]
    width, ff = full.shape[1], pairs[0].shape[1]
    acts_out[:, :width] = full
    out = None
    for b, pair in enumerate(pairs):
        gate = dot(full, pair[0], NT)
        up = dot(full, pair[1], NT)
        gates_out[2 * b] = gate
        gates_out[2 * b + 1] = up
        hidden = (gate * jax.nn.sigmoid(gate) * up).astype(BF16)
        acts_out[:, span(width, ff, b)] = hidden
        if down:
            term = dot(hidden, downs[b][...], NN)
            out = term if out is None else out + term
    if down:
        put_parts(outs[2:], out, rows)


def fwd_layer(chunks, pairs, downs):
    tp, blocks = len(chunks), len(pairs)
    rows, width = chunks[0].shape
    ff = pairs[0].shape[1]
    outs = [sds((tp * rows, width + blocks * lanes(ff)))]
    outs += [sds((2 * blocks, tp * rows, ff), F32)]
    outs += part_shapes(tp, rows, width) if downs else []
    weights = [*pairs, *downs]
    flops = 2 * tp * rows * sum(w.size for w in weights)
    body = functools.partial(fwd_body, tp, blocks, bool(downs))
    res = call(body, outs, [*chunks, *weights], flops)
    return res[:2], res[2:]


def down_body(blocks, acts, *refs):
    downs, outs = refs[:blocks], refs[blocks:]
    ff, width = downs[0].shape
    out = None
    for b in range(blocks):
        term = dot(acts[:, span(width, ff, b)], downs[b][...], NN)
        out = term if out is None else out + term
    put_parts(outs, out, outs[0].shape[0])


def down_layer(acts, downs, tp):
    tokens, width = acts.shape[0], downs[0].shape[1]
    flops = 2 * tokens * sum(w.size for w in downs)
    body = functools.partial(down_body, len(downs))
    return call(body, part_shapes(tp, tokens // tp, width), [acts, *downs], flops)


def join_body(*refs):
    x_ref, own = refs[:2]
    parts, (x_out, n_out) = refs[2:-2], refs[-2:]
    total = own[...]
    for part in parts:
        total = total + part[...].astype(F32)
    x = (x_ref[...].astype(F32) + total).astype(BF16)
    x_out[...] = x
    xf = x.astype(F32)
    n_out[...] = (xf * rows_scale(xf)).astype(BF16)


def join(x, own, parts):
    return call(join_body, [sds(x.shape), sds(x.shape)], [x, own, *parts], 20 * x.size)


def gather_body(*refs):
    refs[-1][...] = jnp.concatenate([c[...] for c in refs[:-1]], axis=0)


def gather(chunks):
    rows, width = chunks[0].shape
    return call(gather_body, [sds((len(chunks) * rows, width))], chunks, 1 << 20)[0]


def bwd_body(tp, blocks, last, grad_ref, gates, *refs):
    downs, refs = refs[:blocks], refs[blocks:]
    pairs, outs = ((), refs) if last else (refs[:blocks], refs[blocks:])
    grad = grad_ref[...]
    rows = grad.shape[0] // tp
    acts_out = outs[0]
    ff = downs[0].shape[0]
    d_norm = None
    for b, down in enumerate(downs):
        d_hidden = dot(grad, down[...], NT)
        gate, up = gates[2 * b], gates[2 * b + 1]
        sig = jax.nn.sigmoid(gate)
        d_gate = (d_hidden * up * sig * (1.0 + gate * (1.0 - sig))).astype(BF16)
        d_up = (d_hidden * (gate * sig)).astype(BF16)
        acts_out[:, span(0, ff, 2 * b)] = d_gate
        acts_out[:, span(0, ff, 2 * b + 1)] = d_up
        if not last:
            term = dot(d_gate, pairs[b][0], NN) + dot(d_up, pairs[b][1], NN)
            d_norm = term if d_norm is None else d_norm + term
    if not last:
        put_parts(outs[1:], d_norm, rows)


def bwd_layer(grad, gates, pairs, downs, tp, last):
    blocks = len(downs)
    rows, width = grad.shape[0] // tp, grad.shape[1]
    outs = [sds((tp * rows, 2 * blocks * lanes(gates.shape[-1])))]
    outs += [] if last else part_shapes(tp, rows, width)
    weights = [*downs] if last else [*downs, *pairs]
    flops = 2 * tp * rows * sum(w.size for w in weights)
    res = call(functools.partial(bwd_body, tp, blocks, last), outs, [grad, gates, *weights], flops)
    return res[0], res[1:]


def back_body(*refs):
    g_ref, x_ref, own = refs[:3]
    parts, out = refs[3:-1], refs[-1]
    d_norm = own[...]
    for part in parts:
        d_norm = d_norm + part[...].astype(F32)
    xf = x_ref[...].astype(F32)
    rinv = rows_scale(xf)
    mean = jnp.mean(d_norm * xf, axis=-1, keepdims=True)
    d_x = g_ref[...].astype(F32) + rinv * d_norm - xf * (rinv * rinv * rinv) * mean
    out[...] = d_x.astype(BF16)


def back(grad, x, own, parts):
    return call(back_body, [sds(x.shape)], [grad, x, own, *parts], 20 * x.size)[0]


def wgrad_body(sources, stages, base, stage_ref, *refs):
    outs = refs[2 * sources * stages :]
    blocks, _, ff, width = outs[0].shape
    kinds = len(outs)
    stage = stage_ref[0]

    def value(side, source, at):
        picked = None
        for s in range(stages):
            one = refs[(side * sources + source) * stages + s][:, at]
            picked = one if picked is None else jnp.where(stage == s, one, picked)
        return picked

    rights = [value(1, source, slice(0, width)) for source in range(sources)]
    for b in range(blocks):
        for kind in range(kinds):
            total = None
            for source in range(sources):
                left = value(0, source, span(base, ff, kinds * b + kind))
                term = dot(left, rights[source], TN)
                total = term if total is None else total + term
            outs[kind][b, 0] = total.astype(BF16)


def wgrad(stage, shape, kinds, base, lefts, rights):
    sources, stages = len(lefts), len(lefts[0])
    args = [v for side in (lefts, rights) for source in side for v in source]
    flops = 2 * sources * args[0].shape[0] * math.prod(shape) * kinds
    return pl.pallas_call(
        functools.partial(wgrad_body, sources, stages, base),
        out_shape=[sds(shape)] * kinds,
        in_specs=[pl.BlockSpec(memory_space=pltpu.SMEM)] + [VMEM] * len(args),
        out_specs=[VMEM] * kinds,
        compiler_params=pltpu.CompilerParams(vmem_limit_bytes=32 << 20),
        cost_estimate=pl.CostEstimate(flops=flops, bytes_accessed=flops // 512, transcendentals=0),
    )(stage.astype(jnp.int32).reshape(1), *args)


def tile_rows(size, most=176):
    return max(r for r in range(16, most + 1, 16) if size % r == 0)


def settle_body(flip, blocks, kind, w_ref, own, *refs):
    other, out = (refs[0], refs[1]) if blocks == 2 else (None, refs[0])
    size = own.shape[-2]
    step = tile_rows(size, 48)
    for d in range(out.shape[0]):
        for b in range(blocks):
            h = blocks - 1 - b if flip else b

            @pl.loop(0, size // step)
            def _(i):
                at = pl.ds(pl.multiple_of(i * step, 16), step)
                to = pl.ds(pl.multiple_of(h * size + i * step, 16), step)
                g = own[b, d, 0, at, :].astype(F32)
                if other is not None:
                    g = g + other[blocks - 1 - b, d, 0, at, :].astype(F32)
                w = w_ref[d, kind, to, :].astype(F32)
                out[d, to, :] = (w - INNER_LR * g).astype(BF16)


def settle(w, kind, own, others, flip):
    depth, _, size, width = w.shape
    body = functools.partial(settle_body, flip, own.shape[0], kind)
    outs = [sds((depth, size, width))]
    return call(body, outs, [w, own, *others], 4 * depth * size * width, 16 << 20)[0]


def update_body(replicas, group, info, *refs):
    inners, others = refs[:group], refs[group : 2 * group]
    outer_ref, moment_ref = refs[2 * group : 2 * group + 2]
    new_out, outer_out, moment_out = refs[-3:]
    core, chosen = info[0], info[1] == 1

    @pl.loop(0, outer_ref.shape[2] // 16)
    def _(i):
        at = pl.ds(pl.multiple_of(i * 16, 16), 16)
        inner, other = inners[0][0, at, :], others[0][0, at, :]
        for g in range(1, group):
            inner = jnp.where(core == g, inners[g][0, at, :], inner)
            other = jnp.where(core == g, others[g][0, at, :], other)
        outer, moment = outer_ref[0, 0, at, :], moment_ref[0, 0, at, :]
        mean = outer - (inner.astype(F32) + other.astype(F32)) / replicas
        next_moment = MOMENTUM * moment + mean
        next_outer = outer - OUTER_LR * (mean + MOMENTUM * next_moment)
        new_out[0, 0, at, :] = jnp.where(chosen, next_outer.astype(BF16), inner)
        outer_out[0, 0, at, :] = jnp.where(chosen, next_outer, outer)
        moment_out[0, 0, at, :] = jnp.where(chosen, next_moment, moment)


def update(info, kind, replicas, inners, others, outer, moment, done):
    group = len(inners)
    depth, kinds, size, width = outer.shape
    rows = tile_rows(size)

    def member(g):
        def at(d, i, info):
            mine = info[0] == g
            return (jnp.where(mine, d, 0), jnp.where(mine, i, 0), 0)

        return pl.BlockSpec((1, rows, width), at)

    whole = pl.BlockSpec((1, 1, rows, width), lambda d, i, info: (d, kind, i, 0))
    specs = [member(g) for g in range(group)] * 2 + [whole] * 2
    specs += [pl.BlockSpec(memory_space=pl.ANY)] * len(done)
    first = 1 + 2 * group + 2
    return pl.pallas_call(
        functools.partial(update_body, replicas, group),
        out_shape=[sds(outer.shape), sds(outer.shape, F32), sds(outer.shape, F32)],
        grid_spec=pltpu.PrefetchScalarGridSpec(
            num_scalar_prefetch=1,
            grid=(depth, size // rows),
            in_specs=specs,
            out_specs=[whole] * 3,
        ),
        input_output_aliases={first + i: i for i in range(len(done))},
        compiler_params=pltpu.CompilerParams(vmem_limit_bytes=67000000),
        cost_estimate=pl.CostEstimate(
            flops=10 * outer.size // kinds,
            bytes_accessed=22 * outer.size // kinds,
            transcendentals=0,
        ),
    )(info, *inners, *others, outer, moment, *done)


def after(value, *others):
    return lax.optimization_barrier((value, others))[0]


def spread(value):
    tp = lax.axis_size("tp")
    return [value] + [
        lax.ppermute(value, "tp", [(i, (i + k) % tp) for i in range(tp)]) for k in range(1, tp)
    ]


def collect(parts):
    tp = lax.axis_size("tp")
    return [
        lax.ppermute(parts[k], "tp", [(i, (i - k) % tp) for i in range(tp)]) for k in range(1, tp)
    ]


def choose(index, values):
    out = values[0]
    for i, value in enumerate(values[1:], 1):
        out = jnp.where(index == i, value, out)
    return out


def shards(
    token_ids,
    embed,
    w_in,
    w_down,
    outer_in,
    outer_down,
    moment_in,
    moment_down,
    cotangent,
    fragment,
):
    sections = lax.axis_size("section")
    section = lax.axis_index("section")
    replicas = lax.axis_size("rep")
    group = 2 if sections % 2 == 0 else 1
    stages = sections // group
    stage, core = section // group, section % group
    shifts = range(1, stages)
    width = embed.shape[1]
    even = core == 0

    def swap(value):
        return lax.ppermute(value, "section", [(s, s ^ 1) for s in range(sections)])

    def shift(value, j):
        pairs = [(s, (s + j * group) % sections) for s in range(sections)]
        return lax.ppermute(value, "section", pairs)

    def to_member(value, member):
        pairs = [(s * group + 1 - member, s * group + member) for s in range(stages)]
        return lax.ppermute(value, "section", pairs)

    pairs = jnp.swapaxes(w_in[0], -1, -2)
    downs = w_down[0]
    depth = pairs.shape[0]
    ff = downs.shape[1]
    block = ff // group

    def cut(value, index):
        return lax.dynamic_slice_in_dim(value, index * block, block, value.ndim - 2)

    own = [pairs, downs]
    if group == 2:
        mine = [cut(w, core) for w in own]
        theirs = [cut(w, 1 - core) for w in own]
        away = [swap(w) for w in theirs]
        pair_first = jnp.where(even, mine[0], away[0])
        mine, away = after((mine, away), pair_first)
        homes = [
            [pair_first, jnp.where(even, mine[1], away[1])],
            [jnp.where(even, a, m) for m, a in zip(mine, away)],
        ]
    else:
        theirs, homes = own, [own]
    gathered = [[None, None] for _ in homes]

    def gather_weights(g, kind, ready):
        w = after(homes[g][kind], ready)
        gathered[g][kind] = [w] + [shift(w, j) for j in shifts]

    gather_weights(0, 0, theirs)

    def layer_weights(s, g, kind, ready):
        parts = gathered[g][kind]
        parts = [parts[0]] + [after(w, ready) for w in parts[1:]]
        ordered = choose((stage - s) % stages, parts)
        both = [ordered] + ([swap(ordered)] if group == 2 else [])
        return [[w[d] for w in both] for d in range(depth)]

    ids = token_ids[0].reshape(stages, group, -1)
    rows = ids.shape[-1]
    ids = lax.dynamic_slice_in_dim(jnp.concatenate([ids, ids], axis=0), stage, stages, 0)
    ids = lax.dynamic_slice_in_dim(jnp.concatenate([ids, ids], axis=1), core, group, 1)
    ids = jnp.swapaxes(ids, 0, 1).reshape(-1)
    vocab_part = embed.shape[0]
    local_ids = after(ids, *theirs, homes[0][0]) - section * vocab_part
    inside = (local_ids >= 0) & (local_ids < vocab_part)
    looked = jnp.take(embed, jnp.clip(local_ids, 0, vocab_part - 1), axis=0)
    looked = jnp.where(inside[:, None], looked, jnp.zeros((), BF16))
    if group == 2:
        split = stages * rows
        looked = looked[:split] + swap(looked[split:])
    gather_weights(0, 1, looked)
    seeds = cotangent[0].reshape(-1, width)
    grad = lax.dynamic_slice_in_dim(seeds, section * rows, rows, 0)
    seed_chunks = spread(grad)
    looks = [shift(looked[j * rows : (j + 1) * rows], j) for j in shifts]
    for g in range(1, group):
        gather_weights(g, 0, looked)
        gather_weights(g, 1, looked)
    x, normed = norm([looked[:rows]] + looks)

    count = stages * group * depth
    saved, xs, layers = [], [], []
    for l in range(count):
        s, g, d = l // (group * depth), l // depth % group, l % depth
        xs.append(x)
        chunks = spread(normed)
        if d == 0:
            ready = normed if l == 0 else chunks if l < group * depth else before
            by_kind = [layer_weights(s, g, 0, ready), layer_weights(s, g, 1, chunks)]
        before = chunks
        if l == 0:
            kept, _ = fwd_layer(chunks, by_kind[0][d], [])
            parts = down_layer(kept[0], by_kind[1][d], len(chunks))
        else:
            downs_used = by_kind[1][d] if l < count - 1 else []
            kept, parts = fwd_layer(chunks, by_kind[0][d], downs_used)
        layers.append((by_kind[0][d], by_kind[1][d]))
        saved.append(kept)
        if l < count - 1:
            collected = collect(parts)
            x, normed = join(x, parts[0], collected)

    def to_home(value, s):
        out = [value]
        for j in shifts:
            t = (s + j) % stages
            pairs = [(t * group + g, s * group + g) for g in range(group)]
            out.append(lax.ppermute(value, "section", pairs))
        return out

    acts = []
    for l in range(count):
        acts.append([to_home(saved[l][0], l // (group * depth))])

    def grads_of(g, pair, ready):
        sets = []
        for d in range(depth):
            of = [acts[(s * group + g) * depth + d] for s in range(stages)]
            kinds = [[[a[kind][j] for a in of] for j in range(stages)] for kind in range(3 if pair else 2)]
            kinds[-1][1:] = [[after(v, ready) for v in one] for one in kinds[-1][1:]]
            shape = (group, 1, block, width)
            if pair:
                sets.append(wgrad(stage, shape, 2, 0, kinds[2], kinds[0]))
            else:
                sets.append(wgrad(stage, shape, 1, width, kinds[0], kinds[1]))
        out = []
        for parts in zip(*sets):
            own = jnp.stack(parts, axis=1)
            out.append((own, [to_member(own, g)] if group == 2 else []))
        return out

    sums = {}
    for l in reversed(range(count)):
        s, g = l // (group * depth), (l + 1) // depth
        gates = saved[l][1]
        chunks = seed_chunks if l == count - 1 else spread(grad)
        if l == group * depth - 1:
            gates = after(gates, *[v for a in acts for v in a[0][1:]])
        whole = gather(chunks)
        acts[l].append(to_home(whole, s))
        if (l + 1) % depth == 0 and 0 < g < group:
            sums[g, True] = grads_of(g, True, grad)
            gates = after(gates, sums[g, True][0][0])
        late, parts = bwd_layer(whole, gates, *layers[l], len(chunks), l == 0)
        acts[l].append(to_home(late, s))
        if l < group * depth and l % depth == 0:
            sums[l // depth, False] = grads_of(l // depth, False, late)
        if l > 0:
            collected = collect(parts)
            grad = back(grad, xs[l], parts[0], collected)

    starts = [pairs, downs[:, None]]

    def exchange(inner, member):
        if replicas != 2:
            every = lax.all_gather(inner, "rep", axis=0).astype(F32)
            return jnp.sum(every, axis=0) - inner.astype(F32)
        ring = [
            ((s * group + member) * 2 + r, (s * group + member) * 2 + 1 - r)
            for s in range(stages)
            for r in range(2)
        ]
        return lax.ppermute(inner, ("section", "rep"), ring)

    inners, others = [[], [], []], [[], [], []]
    sums[0, True] = grads_of(0, True, acts[0][2][0])
    for g in reversed(range(group)):
        for j in (2, 0, 1):
            own, away = sums[g, j < 2][j % 2]
            inner = settle(starts[j // 2], j % 2, own, away, g > 0)
            inners[j].insert(0, inner)
            others[j].insert(0, exchange(inner, g))

    info = jnp.stack([core, lax.dynamic_index_in_dim(fragment, section, 0, keepdims=False)])

    def finish(kind, first, outer, moment, done):
        at = kind - first
        return update(info, at, replicas, inners[kind], others[kind], outer, moment, done)

    flip = lambda v: jnp.swapaxes(v, -1, -2)
    outer_in, moment_in = flip(outer_in), flip(moment_in)
    outer_down, moment_down = outer_down[:, None], moment_down[:, None]
    new_down, next_down, next_m_down = finish(2, 2, outer_down, moment_down, [])
    outer_in, moment_in = after((outer_in, moment_in), next_down)
    done = finish(0, 0, outer_in, moment_in, [])
    new_in, next_in, next_m_in = finish(1, 0, outer_in, moment_in, done)
    return (
        flip(new_in)[None],
        new_down[None, :, 0],
        flip(next_in),
        next_down[:, 0],
        flip(next_m_in),
        next_m_down[:, 0],
    )


def solution(mesh):
    return jax.shard_map(
        shards,
        mesh=mesh,
        in_specs=(
            P("rep", None, "tp"),
            P("section", None),
            P("rep", "section", None, None, "tp"),
            P("rep", "section", "tp", None),
            P("section", None, None, "tp"),
            P("section", "tp", None),
            P("section", None, None, "tp"),
            P("section", "tp", None),
            P("rep", None, "tp", None),
            P(),
        ),
        out_specs=(
            P("rep", "section", None, None, "tp"),
            P("rep", "section", "tp", None),
            P("section", None, None, "tp"),
            P("section", "tp", None),
            P("section", None, None, "tp"),
            P("section", "tp", None),
        ),
        check_vma=False,
    )
```
